32 devices in a mesh: replica: 8 (over z, y), model: 4 (over x, core).
Axes of the slice: x: 2, y: 2, z: 4, core: 2. Of those that a mesh axis runs over, the one named last changes fastest.
Arguments:
- partial_up: float32 [8, 1024, 4096], P('replica', None, 'model'), may hold values from -4 to 4
- partial_down: float32 [8, 4096, 1024], P('replica', 'model'), may hold values from -4 to 4
- partial_norm: float32 [8, 1024], P('replica'), may hold values from -8 to 8
- partial_bias: float32 [8, 1024], P('replica'), may hold values from -8 to 8
- master_up: float32 [1024, 4096], P('replica', 'model'), may hold values from -0.1875 to 0.1875
- master_down: float32 [4096, 1024], P('model', 'replica'), may hold values from -0.09375 to 0.09375
- master_norm: float32 [1024], P('replica'), may hold values from 0.25 to 1.75
- master_bias: float32 [1024], P('replica'), may hold values from -3 to 3
- memory_up: float32 [1024, 4096], P('replica', 'model'), may hold values from 0.05 to 0.8
- memory_down: float32 [4096, 1024], P('model', 'replica'), may hold values from 0.05 to 0.8
- memory_norm: float32 [1024], P('replica'), may hold values from 0.05 to 0.8
- memory_bias: float32 [1024], P('replica'), may hold values from 0.05 to 0.8
Outputs:
- compute_up: bfloat16 [1024, 4096], P(None, 'model')
- compute_down: bfloat16 [4096, 1024], P('model')
- compute_norm: bfloat16 [1024], replicated
- compute_bias: bfloat16 [1024], replicated
- stepped_up: float32 [1024, 4096], P('replica', 'model')
- stepped_down: float32 [4096, 1024], P('model', 'replica')
- stepped_norm: float32 [1024], P('replica')
- stepped_bias: float32 [1024], P('replica')
- state_new_up: float32 [1024, 4096], P('replica', 'model')
- state_new_down: float32 [4096, 1024], P('model', 'replica')
- state_new_norm: float32 [1024], P('replica')
- state_new_bias: float32 [1024], P('replica')
The draws below stay inside these ranges and needn't reach their ends.
All inputs are finite; a program needn't handle non-finite values.
Results may differ from the reference program's by a relative error of at most 0.001.
Values may be sent and summed in bfloat16 or wider, within the bound.
No kernel may reach another device: no remote copies, remote signals or barrier semaphores. Data moves between devices by JAX's collectives and lax.ppermute only.
A program may use at most 128 MiB of HBM per device.

```python
import jax
import jax.numpy as jnp
from jax import lax

WIDTH = 1024
INNER = 4096
REPLICAS = 8


def spiked(result, key, source, target, parts, factor):
    owner, partner = [(jnp.arange(result.shape[dim]) // (result.shape[dim] // parts)).reshape([-1 if axis == dim else 1 for axis in range(result.ndim)]) for dim in (source, target)]
    chosen = jax.random.permutation(key, parts)[partner]
    strong = (owner == chosen) | (owner == (partner + parts // 2) % parts)
    return jnp.where(strong, factor * result, result)


def steps_of(own_key, extent, split, low, high):
    gain = 1.0
    for dim, shards_of in split:
        heights = jax.random.uniform(jax.random.fold_in(jax.random.fold_in(own_key, 6), dim), (shards_of,), jnp.float32, low / len(split), high / len(split))
        gain = gain * jnp.repeat(jnp.exp(heights), extent[dim] // shards_of).reshape((-1,) + (1,) * (len(extent) - 1 - dim))
    return gain


def bell_draw(own_key, extent, width, limit, shards=(), kind=jnp.bfloat16):
    factor_of = steps_of(own_key, extent, shards, -0.22, 0.18) if shards else 1.0
    array = jax.random.normal(own_key, extent, jnp.float32) * width * factor_of
    return jnp.minimum(jnp.maximum(array, -limit), limit).astype(kind)


def heavy_noise(rng, extent, width, reach, cuts, heavy, held_as=jnp.bfloat16):
    entries = width * jax.random.normal(rng, extent, jnp.float32)
    if cuts:
        entries = entries * steps_of(rng, extent, cuts, -0.22, 0.18)
    return jnp.clip(spiked(entries, jax.random.fold_in(rng, 3), *heavy), -reach, reach).astype(held_as)


def setup_inputs(seed: int = 0) -> dict:
    arg_keys = jax.random.split(jax.random.key(seed), 13)
    return {
        "partial_up": heavy_noise(arg_keys[0], (REPLICAS, WIDTH, INNER), 0.5, 4.0, ((0, 8), (2, 4)), (0, 1, 8, 2.0), jnp.float32),
        "partial_down": heavy_noise(arg_keys[1], (REPLICAS, INNER, WIDTH), 0.5, 4.0, ((0, 8), (1, 4)), (0, 2, 8, 2.0), jnp.float32),
        "partial_norm": heavy_noise(arg_keys[2], (REPLICAS, WIDTH), 1.0, 8.0, ((0, 8),), (0, 1, 8, 2.0), jnp.float32),
        "partial_bias": heavy_noise(arg_keys[3], (REPLICAS, WIDTH), 1.0, 8.0, ((0, 8),), (0, 1, 8, 2.0), jnp.float32),
        "master_up": bell_draw(arg_keys[4], (WIDTH, INNER), WIDTH ** -0.5, 0.1875, ((0, 8), (1, 4)), jnp.float32),
        "master_down": bell_draw(arg_keys[5], (INNER, WIDTH), INNER ** -0.5, 0.09375, ((0, 4), (1, 8)), jnp.float32),
        "master_norm": jnp.clip(1.0 + 0.15 * jax.random.normal(arg_keys[6], (WIDTH,), jnp.float32), 0.25, 1.75),
        "master_bias": bell_draw(arg_keys[7], (WIDTH,), 0.5, 3.0, ((0, 8),), jnp.float32),
        "memory_up": jnp.clip(0.05 + 0.75 * jax.random.uniform(arg_keys[8], (WIDTH, INNER), jnp.float32) ** steps_of(arg_keys[8], (WIDTH, INNER), ((0, 8), (1, 4)), -0.2, 0.2), 0.05, 0.8),
        "memory_down": jnp.clip(0.05 + 0.75 * jax.random.uniform(arg_keys[9], (INNER, WIDTH), jnp.float32) ** steps_of(arg_keys[9], (INNER, WIDTH), ((0, 4), (1, 8)), -0.2, 0.2), 0.05, 0.8),
        "memory_norm": jnp.clip(0.05 + 0.75 * jax.random.uniform(arg_keys[10], (WIDTH,), jnp.float32) ** steps_of(arg_keys[10], (WIDTH,), ((0, 8),), -0.2, 0.2), 0.05, 0.8),
        "memory_bias": jnp.clip(0.05 + 0.75 * jax.random.uniform(arg_keys[11], (WIDTH,), jnp.float32) ** steps_of(arg_keys[11], (WIDTH,), ((0, 8),), -0.2, 0.2), 0.05, 0.8),
    }


learn_rate = 0.05
hold_rate = 0.9

def reference(partial_up, partial_down, partial_norm, partial_bias, master_up, master_down, master_norm, master_bias, memory_up, memory_down, memory_norm, memory_bias):
    mean_up = lax.optimization_barrier(jnp.sum(partial_up.astype(jnp.float32), axis=0)) * REPLICAS ** (-0.5)
    mean_down = lax.optimization_barrier(jnp.sum(partial_down.astype(jnp.float32), axis=0)) * REPLICAS ** (-0.5)
    mean_norm = lax.optimization_barrier(jnp.sum(partial_norm.astype(jnp.float32), axis=0)) * REPLICAS ** (-0.5)
    mean_bias = lax.optimization_barrier(jnp.sum(partial_bias.astype(jnp.float32), axis=0)) * REPLICAS ** (-0.5)
    state_new_up = hold_rate * memory_up + (1.0 - hold_rate) * mean_up * mean_up
    stepped_up = master_up - learn_rate * mean_up * lax.rsqrt(state_new_up + 1e-06)
    state_new_down = hold_rate * memory_down + (1.0 - hold_rate) * mean_down * mean_down
    stepped_down = master_down - learn_rate * mean_down * lax.rsqrt(state_new_down + 1e-06)
    state_new_norm = hold_rate * memory_norm + (1.0 - hold_rate) * mean_norm * mean_norm
    stepped_norm = master_norm - learn_rate * mean_norm * lax.rsqrt(state_new_norm + 1e-06)
    state_new_bias = hold_rate * memory_bias + (1.0 - hold_rate) * mean_bias * mean_bias
    stepped_bias = master_bias - learn_rate * mean_bias * lax.rsqrt(state_new_bias + 1e-06)
    compute_up = stepped_up.astype(jnp.bfloat16)
    compute_down = stepped_down.astype(jnp.bfloat16)
    compute_norm = stepped_norm.astype(jnp.bfloat16)
    compute_bias = stepped_bias.astype(jnp.bfloat16)
    return (compute_up, compute_down, compute_norm, compute_bias, stepped_up, stepped_down, stepped_norm, stepped_bias, state_new_up, state_new_down, state_new_norm, state_new_bias)
```

```python
import jax
import jax.numpy as jnp
from jax import lax
from jax.sharding import PartitionSpec as P

learn_rate = 0.05
hold_rate = 0.9

REDUCE_UP = (0, 1, 2)
REDUCE_DOWN = (1, 0, 2)
GATHER_UP = (2, 1, 0)
GATHER_DOWN = (2, 1, 0)


def step(total, memory, master, rate):
    mean = total * rate
    state = hold_rate * memory + (1.0 - hold_rate) * mean * mean
    return state, master - learn_rate * mean * lax.rsqrt(state + 1e-06)


def swap(value, bit):
    size = lax.axis_size("replica")
    return lax.ppermute(value, "replica", [(r, r ^ (1 << bit)) for r in range(size)])


def scale_of(level):
    return 16.0 / 2**level


def pack(value, level):
    scaled = value * scale_of(level)
    return (scaled * jnp.abs(scaled)).astype(jnp.float16)


def unpack(code, level):
    wide = code.astype(jnp.float32)
    root = jnp.sqrt(jnp.abs(wide)) * (1.0 / scale_of(level))
    return jnp.where(wide < 0.0, -root, root)


def reduce_shares(share, order):
    held = {}

    def partial(mask):
        value = share(mask)
        for level, part in held.get(mask, ()):
            value = value + unpack(part, level)
        return value

    masks = list(range(lax.axis_size("replica")))
    for level, bit in enumerate(order):
        leaving = [m for m in masks if m >> bit & 1]
        masks = [m for m in masks if not m >> bit & 1]
        if level + 1 < len(order):
            turn = order[level + 1]
            groups = [
                [m for m in leaving if m >> turn & 1],
                [m for m in leaving if not m >> turn & 1],
            ]
        else:
            groups = [leaving]
        news = []
        for group in groups:
            got = swap(jnp.stack([pack(partial(m), level) for m in group]), bit)
            for place, m in enumerate(group):
                news.append((m ^ (1 << bit), got[place]))
        for m, part in news:
            held.setdefault(m, []).append((level, part))
    return partial(0)


def gather_shares(share, order):
    held = {0: share}
    for bit in order:
        held.update({m ^ (1 << bit): swap(v, bit) for m, v in held.items()})
    return held


def in_turns(
    partial_up,
    partial_down,
    partial_norm,
    partial_bias,
    master_up,
    master_down,
    master_norm,
    master_bias,
    memory_up,
    memory_down,
    memory_norm,
    memory_bias,
):
    size = lax.axis_size("replica")
    bits = size.bit_length() - 1
    place = lax.axis_index("replica")
    rate = size ** (-0.5)

    share = master_norm.shape[0]
    mine = jnp.stack([master_norm, memory_norm, master_bias, memory_bias])
    laid = lax.dynamic_update_slice(
        jnp.zeros((4, size, share), jnp.float32), mine[:, None], (0, place, 0)
    )
    vectors = jnp.concatenate(
        [
            partial_norm.reshape(1, size, share),
            partial_bias.reshape(1, size, share),
            laid,
        ]
    )
    for bit in range(bits):
        vectors = vectors + swap(vectors, bit)
    states, steppeds = step(
        vectors[:2], vectors[3::2], vectors[2::2], rate
    )
    computes = steppeds.astype(jnp.bfloat16).reshape(2, size * share)
    own = lambda a: lax.dynamic_slice(a, (0, place, 0), (2, 1, share)).reshape(2, share)
    states, steppeds = own(states), own(steppeds)

    rows = master_up.shape[0]
    columns = master_down.shape[1]
    up_share = lambda m: lax.dynamic_slice_in_dim(
        partial_up[0], (place ^ m) * rows, rows, 0
    )
    down_share = lambda m: lax.dynamic_slice_in_dim(
        partial_down[0], (place ^ m) * columns, columns, 1
    )
    total_up = reduce_shares(up_share, REDUCE_UP)
    total_down = reduce_shares(down_share, REDUCE_DOWN)
    state_up, stepped_up = step(total_up, memory_up, master_up, rate)
    state_down, stepped_down = step(total_down, memory_down, master_down, rate)
    parts_up = gather_shares(stepped_up.astype(jnp.bfloat16), GATHER_UP)
    parts_down = gather_shares(stepped_down.astype(jnp.bfloat16), GATHER_DOWN)
    compute_up = jnp.zeros(partial_up.shape[1:], jnp.bfloat16)
    for m, part in parts_up.items():
        compute_up = lax.dynamic_update_slice_in_dim(
            compute_up, part, (place ^ m) * rows, 0
        )
    compute_down = jnp.zeros(partial_down.shape[1:], jnp.bfloat16)
    for m, part in parts_down.items():
        compute_down = lax.dynamic_update_slice_in_dim(
            compute_down, part, (place ^ m) * columns, 1
        )
    return (
        compute_up,
        compute_down,
        computes[0],
        computes[1],
        stepped_up,
        stepped_down,
        steppeds[0],
        steppeds[1],
        state_up,
        state_down,
        states[0],
        states[1],
    )


def by_collectives(
    partial_up,
    partial_down,
    partial_norm,
    partial_bias,
    master_up,
    master_down,
    master_norm,
    master_bias,
    memory_up,
    memory_down,
    memory_norm,
    memory_bias,
):
    place = lax.axis_index("replica")
    rate = lax.axis_size("replica") ** (-0.5)
    whole_norm, whole_bias = lax.psum((partial_norm[0], partial_bias[0]), "replica")
    own = lambda whole, like: lax.dynamic_slice_in_dim(
        whole, place * like.shape[0], like.shape[0]
    )
    totals = (
        lax.psum_scatter(partial_up[0], "replica", scatter_dimension=0, tiled=True),
        lax.psum_scatter(partial_down[0], "replica", scatter_dimension=1, tiled=True),
        own(whole_norm, master_norm),
        own(whole_bias, master_bias),
    )
    memories = (memory_up, memory_down, memory_norm, memory_bias)
    masters = (master_up, master_down, master_norm, master_bias)
    pairs = [step(t, e, a, rate) for t, e, a in zip(totals, memories, masters)]
    computes = [
        lax.all_gather(s.astype(jnp.bfloat16), "replica", axis=d, tiled=True)
        for (_, s), d in zip(pairs, (0, 1, 0, 0))
    ]
    return (*computes, *(s for _, s in pairs), *(e for e, _ in pairs))


def solution(mesh):
    in_specs = (
        P("replica", None, "model"),
        P("replica", "model", None),
        P("replica", None),
        P("replica", None),
        P("replica", "model"),
        P("model", "replica"),
        P("replica"),
        P("replica"),
        P("replica", "model"),
        P("model", "replica"),
        P("replica"),
        P("replica"),
    )
    out_specs = (
        P(None, "model"),
        P("model", None),
        P(),
        P(),
        P("replica", "model"),
        P("model", "replica"),
        P("replica"),
        P("replica"),
        P("replica", "model"),
        P("model", "replica"),
        P("replica"),
        P("replica"),
    )
    body = in_turns if mesh.shape["replica"] == 1 << len(REDUCE_UP) else by_collectives
    return jax.shard_map(
        body, mesh=mesh, in_specs=in_specs, out_specs=out_specs, check_vma=False
    )
```
